32 devices in a mesh: gx: 4 (over z), gy: 4 (over x, core), gz: 2 (over y).
Axes of the slice: x: 2, y: 2, z: 4, core: 2. Of those that a mesh axis runs over, the one named last changes fastest.
Arguments:
- hidden_in: bfloat16 [2048, 4096], P(('gx', 'gy'), 'gz'), may hold values from -40 to 40
- norm_gain: float32 [4096], P('gz'), may hold values from 0.25 to 1.75
- normed_grad: bfloat16 [2048, 4096], P(('gx', 'gy'), 'gz'), may hold values from -64 to 64
- key_grad: bfloat16 [2048, 512], P(('gx', 'gy')), may hold values from -6 to 6
- weight_blocks: bfloat16 [16, 2, 520, 128], P(('gx', 'gy'), 'gz'), may hold values from -0.09375 to 0.09375
- block_count: int32 [2, 16], P('gz'), may hold values from 1 to 520, as said below
Outputs:
- hidden_grad: bfloat16 [2048, 4096], P(('gx', 'gy'), 'gz')
- weight_grad: float32 [16, 2, 520, 128], P(('gx', 'gy'), 'gz')
The draws below stay inside these ranges and needn't reach their ends.
Inputs may be any that keep to these rules, and one draw needn't show every extreme that they name: `block_count`: each row sums to 8192; in each row the owners i * 4 to i * 4 + 3 hold together exactly the blocks i * 2048 to min((i + 1) * 2048, 8192) - 1, and one of them holds exactly 520 blocks.
All inputs are finite; a program needn't handle non-finite values.
Results may differ from the reference program's by a relative error of at most 0.0029.
Values may be sent and summed in bfloat16 or wider, within the bound.
A program may use at most 64 MiB of HBM per device.

```python
import math
import jax
import jax.numpy as jnp
from jax import lax

D = 4096
KVW = 512
TOK_DEV = 128
OUTER = 4
INNER = 4
OWNERS = 16
TOKENS = 2048
QUARTERS = 2
BLOCKS = 8192
GROUPB = 2048
MAXB = 520


def joint_activations(key):
    subkeys = jax.random.split(jax.random.fold_in(key, 7001), 5)
    position = jnp.arange(D, dtype=jnp.float32) / D
    base = jnp.clip(jax.random.normal(subkeys[0], (TOKENS, D), jnp.float32), -4.0, 4.0)
    column = jnp.power(3.0, position) * jnp.exp(jax.random.uniform(subkeys[1], (D,), jnp.float32, math.log(0.6), math.log(1.6)))
    hidden = base * column[None, :]
    coefficient = jax.random.uniform(subkeys[3], (TOKENS, 1), jnp.float32, -1.5, 1.5)
    noise = 0.5 * jnp.clip(jax.random.normal(subkeys[4], (TOKENS, D), jnp.float32), -4.0, 4.0)
    return (hidden, coefficient * hidden + noise)


def draw_hidden_in(key, part):
    hidden, _ = joint_activations(key)
    return hidden.astype(jnp.bfloat16)


def draw_normed_grad(key, part):
    _, cotangent = joint_activations(key)
    return cotangent.astype(jnp.bfloat16)


def draw_block_count(key, part):
    subkeys = jax.random.split(jax.random.fold_in(key, 7002), 2)
    group_ids = jnp.arange(OUTER, dtype=jnp.int32)
    totals = jnp.minimum(GROUPB, BLOCKS - group_ids * GROUPB).astype(jnp.int32)
    totals = jnp.broadcast_to(totals[None, :, None], (QUARTERS, OUTER, 1))
    chosen = jax.random.randint(subkeys[0], (QUARTERS, OUTER, 1), 0, INNER, dtype=jnp.int32)
    member = jnp.arange(INNER, dtype=jnp.int32)[None, None, :]
    is_full = member == chosen
    raw_weight = jax.random.randint(subkeys[1], (QUARTERS, OUTER, INNER), 1, 6, dtype=jnp.int32)
    weights = jnp.where(is_full, 0, raw_weight * raw_weight * raw_weight)
    extra = totals - MAXB - (INNER - 1)
    share = extra * weights // jnp.sum(weights, axis=2, keepdims=True)
    share = jnp.minimum(share, MAXB - 1)
    leftover = extra - jnp.sum(share, axis=2, keepdims=True)
    room = jnp.where(is_full, 0, MAXB - 1 - share)
    before = jnp.cumsum(room, axis=2) - room
    share = share + jnp.clip(leftover - before, 0, room)
    counts = jnp.where(is_full, MAXB, 1 + share)
    return counts.reshape(QUARTERS, OWNERS).astype(jnp.int32)


def block_levels(stream_key, dims, cuts, low, largest):
    factor_of = 1.0
    for dim, blocks in cuts:
        steps = jax.random.uniform(jax.random.fold_in(jax.random.fold_in(stream_key, 6), dim), (blocks,), jnp.float32, low / len(cuts), largest / len(cuts))
        factor_of = factor_of * jnp.repeat(jnp.exp(steps), dims[dim] // blocks).reshape((-1,) + (1,) * (len(dims) - 1 - dim))
    return factor_of


def scatter_about(rng, dims, deviation, most, cuts=(), held_as=jnp.bfloat16):
    loudness = block_levels(rng, dims, cuts, -0.22, 0.18) if cuts else 1.0
    result = jax.random.normal(rng, dims, jnp.float32) * deviation * loudness
    return jnp.minimum(jnp.maximum(result, -most), most).astype(held_as)


def setup_inputs(seed: int = 0) -> dict:
    seeds = jax.random.split(jax.random.key(seed), 7)
    return {
        "hidden_in": draw_hidden_in(jax.random.fold_in(seeds[6], 71), 0),
        "norm_gain": jnp.clip(1.0 + 0.15 * jax.random.normal(seeds[1], (D,), jnp.float32), 0.25, 1.75),
        "normed_grad": draw_normed_grad(jax.random.fold_in(seeds[6], 71), 0),
        "key_grad": scatter_about(seeds[3], (TOKENS, KVW), 1.0, 6.0, ((0, 16),)),
        "weight_blocks": scatter_about(seeds[4], (OWNERS, QUARTERS, MAXB, 128), D ** -0.5, 0.09375, ((0, 16), (1, 2))),
        "block_count": draw_block_count(jax.random.fold_in(seeds[6], 71), 0),
    }


EPS = 1e-06

def block_layout(counts):
    ends = jnp.cumsum(counts).astype(jnp.int32)
    starts = (ends - counts).astype(jnp.int32)
    block_ids = jnp.arange(BLOCKS, dtype=jnp.int32)
    owner = jnp.searchsorted(ends, block_ids, side='right').astype(jnp.int32)
    gather_index = (owner * MAXB + block_ids - starts[owner]).astype(jnp.int32)
    slot_owner = jnp.arange(OWNERS * MAXB, dtype=jnp.int32) // MAXB
    slot_within = jnp.arange(OWNERS * MAXB, dtype=jnp.int32) % MAXB
    valid = slot_within < counts[slot_owner]
    source = jnp.clip(starts[slot_owner] + slot_within, 0, BLOCKS - 1).astype(jnp.int32)
    return (gather_index, source, valid)

def reference(hidden_in, norm_gain, normed_grad, key_grad, weight_blocks, block_count):
    group_rows = D // QUARTERS
    pieces = []
    layouts = []
    for group in range(QUARTERS):
        gather_index, source, valid = block_layout(block_count[group])
        layouts.append((source, valid))
        rows = weight_blocks[:, group].reshape(OWNERS * MAXB, 128)
        pieces.append(rows[gather_index].reshape(group_rows, KVW))
    weight = jnp.concatenate(pieces, axis=0)
    gain = norm_gain.astype(jnp.float32)

    def step(total, items):
        hblock, nblock, kblock = items
        hfloat = hblock.astype(jnp.float32)
        rstd = lax.rsqrt(lax.optimization_barrier(jnp.sum(hfloat * hfloat, axis=1)) / D + EPS)
        normed = (hfloat * rstd[:, None] * gain).astype(jnp.bfloat16)
        total = total + lax.dot_general(normed, kblock, (((0,), (0,)), ((), ())), preferred_element_type=jnp.float32)
        dnorm = nblock.astype(jnp.float32) + lax.dot_general(kblock, weight, (((1,), (1,)), ((), ())), preferred_element_type=jnp.float32)
        proj = lax.optimization_barrier(jnp.sum(gain * dnorm * hfloat, axis=1))
        grad = gain * dnorm * rstd[:, None] - hfloat * (rstd ** 3 * proj / D)[:, None]
        return (total, grad.astype(jnp.bfloat16))
    hsplit = hidden_in.reshape(OWNERS, TOK_DEV, D)
    nsplit = normed_grad.reshape(OWNERS, TOK_DEV, D)
    ksplit = key_grad.reshape(OWNERS, TOK_DEV, KVW)
    dweight, grads = lax.scan(step, jnp.zeros((D, KVW), jnp.float32), (hsplit, nsplit, ksplit))
    outs = []
    for group in range(QUARTERS):
        source, valid = layouts[group]
        flat = dweight[group * group_rows:(group + 1) * group_rows].reshape(BLOCKS, 128)
        padded = jnp.where(valid[:, None], flat[source], jnp.float32(0.0))
        outs.append(padded.reshape(OWNERS, MAXB, 128))
    weight_grad = jnp.stack(outs, axis=1)
    return (grads.reshape(TOKENS, D), weight_grad)
```

```python
import functools
import jax
import jax.numpy as jnp
from jax import lax
from jax.experimental import pallas as pl
from jax.experimental.pallas import tpu as pltpu
from jax.sharding import PartitionSpec as P

EPS = 1e-06
LANE = 128
MESH = pl.DeviceIdType.MESH
VMEM_BUDGET = 48 * 2**20


def owner_windows(group, inner, most, per_row, rows):
    lows, highs = [], []
    for j in range(inner):
        low = max(j, group - (inner - j) * most)
        high = min(min(j * most, group - (inner - j)) + most, group)
        lows.append(low // per_row // 8 * 8)
        highs.append(-(-high // per_row))
    height = -(-max(h - l for l, h in zip(lows, highs)) // 16) * 16
    return [min(low, rows - height) for low in lows], height


def sum_orders(outer):
    table = []
    for a in range(outer):
        up, down = list(range(outer - 1, a, -1)), list(range(a))
        table.append((up + down if len(up) >= len(down) else down + up) + [a])
    return table


def gather_orders(outer):
    table = []
    for a in range(outer):
        row = [a]
        for s in range(1, outer):
            row += [p for p in (a - s, a + s) if 0 <= p < outer]
        table.append(row)
    return table


def fast_kernel(
    dims, lows,
    count_ref, hidden_hbm, gain_ref, ngrad_hbm, key_hbm, wb_hbm,
    hgrad_ref, wgrad_ref,
    hidden_ref, ngrad_ref, wb_ref, kall, wwin, h_send, h_recv, p_send, p_recv,
    feat, grow, gcol, wpad, wflat, dacc, rs_send, rs_recv, dflat,
    sq_send, sq_recv, rrow, pj_acc, pj_recv, py_send, py_recv,
    own_sem, k_ssem, k_rsem, up_ssem, dn_ssem, w_rsem, h_ssem, h_rsem, p_ssem, p_rsem,
    rs_ssem, rs_rsem, r_ssem, r_rsem, pj_ssem, pj_rsem, y_ssem, y_rsem,
):
    outer, inner, model_width, most, per_row, height, pad = dims
    f32, bf16 = jnp.float32, jnp.bfloat16
    a, b, g = lax.axis_index("gx"), lax.axis_index("gy"), lax.axis_index("gz")
    x, c = b // 2, b % 2
    me = a * inner + b
    tokens, rows = hidden_ref.shape
    width = kall.shape[2]
    owners = outer * inner
    span = rows // outer
    chunks = rows // LANE
    last = outer - 1
    low_me = lows[0] + x * (lows[2] - lows[0]) + c * (lows[1] - lows[0]) + x * c * (
        lows[3] - lows[2] - lows[1] + lows[0])
    mid = height // 32 * 16 + (16 if height // 16 % 2 else 0)
    halves = (slice(0, mid), slice(mid, height))
    interior = jnp.logical_and(a > 0, a < last)
    ends = jnp.logical_or(a == 0, a == last)

    def pick(table, k):
        value = jnp.int32(0)
        for j in range(outer):
            value = value + jnp.where(a == j, table[j][k], 0)
        return value

    sum_table, gather_table = sum_orders(outer), gather_orders(outer)

    def peer(k):
        px = 1 - x if k // 2 else x
        pc = 1 - c if k % 2 else c
        return px * 2 + pc

    def slot_of(j):
        return (x if j // 2 == 0 else 1 - x) * 2 + (c if j % 2 == 0 else 1 - c)

    def remote(src, dst, send, recv, gx, gy, gz):
        return pltpu.make_async_remote_copy(
            src_ref=src, dst_ref=dst, send_sem=send, recv_sem=recv,
            device_id=(gx, gy, gz), device_id_type=MESH)

    sends = []

    def start(copy):
        copy.start()
        sends.append((copy, None))
        return copy

    def start_if(cond, copy):
        pl.when(cond)(copy.start)
        sends.append((copy, cond))
        return copy

    own = [
        pltpu.make_async_copy(wb_hbm, wb_ref, own_sem.at[0]),
        pltpu.make_async_copy(hidden_hbm, hidden_ref, own_sem.at[1]),
        pltpu.make_async_copy(key_hbm, kall.at[0], own_sem.at[2]),
        pltpu.make_async_copy(ngrad_hbm, ngrad_ref, own_sem.at[3]),
    ]
    for copy in own:
        copy.start()
    barrier = pltpu.get_barrier_semaphore()
    for k in range(1, inner):
        pl.semaphore_signal(barrier, inc=1, device_id=(a, peer(k), g), device_id_type=MESH)
    pl.semaphore_signal(barrier, inc=1, device_id=(a, b, 1 - g), device_id_type=MESH)

    @pl.when(a < last)
    def _():
        pl.semaphore_signal(barrier, inc=1, device_id=(a + 1, b, g), device_id_type=MESH)

    @pl.when(a > 0)
    def _():
        pl.semaphore_signal(barrier, inc=1, device_id=(a - 1, b, g), device_id_type=MESH)

    begin = jnp.int32(0)
    count = jnp.int32(0)
    for o in range(owners):
        value = count_ref[0, o]
        begin = begin + jnp.where(o < me, value, 0)
        count = count + jnp.where(me == o, value, 0)
    offset = jnp.clip(begin - (a * span + low_me) * per_row, 0, pad)
    flat_rows = height * per_row
    slot = lax.broadcasted_iota(jnp.int32, (most, LANE), 0)
    wpad[...] = jnp.zeros_like(wpad)
    own[0].wait()
    wpad[pad:pad + most, :] = jnp.where(slot < count, wb_ref[...].astype(f32), 0.0)
    wflat[...] = wpad[pl.ds(pad - offset, flat_rows), :]
    for i in range(per_row):
        wwin[a, :, i * LANE:(i + 1) * LANE] = wflat[pl.ds(i, height, stride=per_row), :].astype(bf16)

    own[1].wait()
    squares = jnp.zeros((tokens, LANE), f32)
    for i in range(chunks):
        part = hidden_ref[:, i * LANE:(i + 1) * LANE].astype(f32)
        squares = squares + part * part
    row_sum = jnp.sum(squares, axis=1, keepdims=True)
    sq_send[...] = jnp.broadcast_to(row_sum, (tokens, LANE)).T[0:8, :]

    own[2].wait()
    pl.semaphore_wait(barrier, inner + jnp.where(a < last, 1, 0) + jnp.where(a > 0, 1, 0))

    sq_copy = start(remote(sq_send, sq_recv, y_ssem.at[0], y_rsem.at[0], a, b, 1 - g))
    k_copy = {k: start(remote(kall.at[0], kall.at[k], k_ssem.at[k], k_rsem.at[k], a, peer(k), g))
              for k in (2, 1)}

    def gather(piece, h, up):
        part = wwin.at[piece, halves[h]]
        send = (up_ssem if up else dn_ssem).at[piece, h]
        return remote(part, part, send, w_rsem.at[piece, h], a + 1 if up else a - 1, b, g)

    for h in range(2):
        start_if(a < last, gather(a, h, True))
        start_if(a > 0, gather(a, h, False))

    h_copy, r_copy = {}, {}
    for i in range(outer):
        z = pick(sum_table, i)
        for q in range(span // LANE):
            cols = pl.ds(pl.multiple_of(z * span + q * LANE, LANE), LANE)
            feat[q * LANE:(q + 1) * LANE, :] = hidden_ref[:, cols].astype(f32).T
        for j in range(inner):
            h_send[z, j] = feat[lows[j]:lows[j] + height, :].astype(bf16)
        for k in (2, 3, 1):
            h_copy[i, k] = start(remote(
                h_send.at[z, peer(k)], h_recv.at[z, k], h_ssem.at[z, k], h_rsem.at[z, k], a, peer(k), g))
        if i == 0:
            sq_copy.wait_recv()
            rrow[0] = lax.rsqrt((sq_send[...] + sq_recv[...]) / model_width + EPS)
            for k in (2, 3, 1):
                r_copy[k] = start(remote(
                    rrow.at[0], rrow.at[k], r_ssem.at[k], r_rsem.at[k], a, peer(k), g))

    rstd = jnp.broadcast_to(rrow[0, 0:1, :], (tokens, LANE)).T[:, 0:1]
    for i in range(chunks):
        cols = slice(i * LANE, (i + 1) * LANE)
        gcol[cols, :] = jnp.broadcast_to(gain_ref[:, cols], (LANE, LANE)).T
    own[3].wait()
    local = jnp.zeros((tokens, LANE), f32)
    for i in range(chunks):
        cols = slice(i * LANE, (i + 1) * LANE)
        local = local + gain_ref[:, cols] * ngrad_ref[:, cols].astype(f32) * hidden_ref[:, cols].astype(f32)
    local_sum = jnp.sum(local, axis=1, keepdims=True)
    py_send[...] = jnp.broadcast_to(local_sum, (tokens, LANE)).T[0:8, :]

    k_copy[2].wait_recv()
    k_copy[3] = start(remote(kall.at[2], kall.at[3], k_ssem.at[3], k_rsem.at[3], a, peer(1), g))

    def gather_step(s):
        below, above = a - s >= 0, a + s <= last
        for h in range(2):
            @pl.when(below)
            def _():
                gather(a - s, h, True).wait_recv()
            start_if(jnp.logical_and(below, a < last), gather(a - s, h, True))

            @pl.when(above)
            def _():
                gather(a + s, h, False).wait_recv()
            start_if(jnp.logical_and(above, a > 0), gather(a + s, h, False))

    def keys():
        return kall[...].reshape(inner * tokens, width)

    def p_copy(z, k):
        return remote(p_send.at[z, k], p_recv.at[z, k], p_ssem.at[z, k], p_rsem.at[z, k], a, peer(k), g)

    def project(z):
        product = lax.dot_general(
            wwin[z], keys(), (((1,), (1,)), ((), ())), preferred_element_type=f32)
        p_recv[z, 0] = product[:, 0:tokens].astype(bf16)
        for k in (2, 3, 1):
            p_send[z, k] = product[:, k * tokens:(k + 1) * tokens].astype(bf16)
            p_copy(z, k).start()

    def gain_rows(z):
        return gcol[pl.ds(pl.multiple_of(z * span + low_me, 8), height), :]

    def hidden_rows(z, k):
        return (h_send[z, b] if k == 0 else h_recv[z, k]).astype(f32)

    def partial(i):
        z = pick(sum_table, i)
        gains = gain_rows(z)
        for k in range(1, inner):
            h_copy[i, k].wait_recv()
        normed = [(hidden_rows(z, k) * rrow[k, 0:1, :] * gains).astype(bf16) for k in range(inner)]
        dacc[i] = jnp.dot(jnp.concatenate(normed, axis=1), keys(), preferred_element_type=f32)

    def sum_copy(i, h):
        z = pick(sum_table, i)
        up = (z > a).astype(jnp.int32)
        place = z + (1 - up) * outer
        return remote(rs_send.at[i, halves[h]], rs_recv.at[place, halves[h]],
                      rs_ssem.at[i, h], rs_rsem.at[place, h], a + 2 * up - 1, b, g)

    def sum_send(i, h):
        rs_send[i, halves[h]] = dacc[i, halves[h]].astype(bf16)
        sum_copy(i, h).start()

    def sum_ends(i):
        @pl.when(ends)
        def _():
            for h in range(2):
                sum_send(i, h)

    def sum_wait(place, h):
        part = rs_recv.at[place, halves[h]]
        remote(part, part, rs_ssem.at[0, h], rs_rsem.at[place, h], a, b, 1 - g).wait_recv()

    def sum_interior(i):
        @pl.when(interior)
        def _():
            z = pick(sum_table, i)
            place = z + jnp.where(z > a, 0, outer)
            for h in range(2):
                sum_wait(place, h)
                dacc[i, halves[h]] += rs_recv[place, halves[h]].astype(f32)
                sum_send(i, h)

    def inner_products(z, first):
        gains = gain_rows(z)
        for k in range(inner):
            part = (p_recv[z, 0] if k == 0 else p_send[z, k]).astype(f32)
            term = part * hidden_rows(z, k) * gains
            term = jnp.sum(term.reshape(height // 8, 8, LANE), axis=0)
            pj_acc[k] = term if first else pj_acc[k] + term

    def accumulate(i):
        z = pick(gather_table, i)
        for k in range(1, inner):
            p_copy(z, k).wait_recv()
        feat[...] = jnp.zeros_like(feat)
        for j in range(inner):
            feat[lows[j]:lows[j] + height, :] += p_recv[z, slot_of(j)].astype(f32)
        for q in range(span // LANE):
            cols = pl.ds(pl.multiple_of(z * span + q * LANE, LANE), LANE)
            dnorm = ngrad_ref[:, cols].astype(f32) + feat[q * LANE:(q + 1) * LANE, :].T
            grow[:, cols] = gain_ref[:, cols] * dnorm * rstd

    def project_step(s):
        for piece, there in ((a - s, a - s >= 0), (a + s, a + s <= last)):
            @pl.when(there)
            def _():
                project(piece)

    gather_step(1)
    k_copy[1].wait_recv()
    k_copy[3].wait_recv()
    project(a)
    for k in range(1, inner):
        r_copy[k].wait_recv()
    partial(0)
    sum_ends(0)
    project_step(1)
    partial(1)
    sum_ends(1)
    for s in range(2, last):
        gather_step(s)
        project_step(s)
    for i in range(2, last):
        partial(i)
        sum_ends(i)
    partial(last)
    inner_products(a, True)
    sum_interior(0)
    gather_step(last)
    project_step(last)
    for i in range(1, outer):
        inner_products(pick(gather_table, i), False)
    pj_copy = {k: start(remote(pj_acc.at[k], pj_recv.at[k], pj_ssem.at[k], pj_rsem.at[k], a, peer(k), g))
               for k in (2, 3, 1)}
    accumulate(0)
    for i in range(1, last):
        sum_interior(i)
        accumulate(i)
    for k in range(1, inner):
        pj_copy[k].wait_recv()
    first_row = lax.broadcasted_iota(jnp.int32, (8, LANE), 0) == 0
    py_send[...] = (jnp.where(first_row, py_send[...], 0.0) + pj_acc[0]
                    + pj_recv[1] + pj_recv[2] + pj_recv[3])
    py_copy = start(remote(py_send, py_recv, y_ssem.at[1], y_rsem.at[1], a, b, 1 - g))
    accumulate(last)
    py_copy.wait_recv()
    proj_row = jnp.sum(py_send[...] + py_recv[...], axis=0, keepdims=True)
    proj_all = jnp.broadcast_to(proj_row, (tokens, LANE)).T[:, 0:1]
    scale = rstd * rstd * rstd * proj_all / model_width
    for i in range(chunks):
        cols = slice(i * LANE, (i + 1) * LANE)
        hgrad_ref[:, cols] = (grow[:, cols] - hidden_ref[:, cols].astype(f32) * scale).astype(bf16)

    for h in range(2):
        @pl.when(a > 0)
        def _():
            sum_wait(a, h)
            dacc[last, halves[h]] += rs_recv[a, halves[h]].astype(f32)

        @pl.when(a < last)
        def _():
            sum_wait(a + outer, h)
            dacc[last, halves[h]] += rs_recv[a + outer, halves[h]].astype(f32)
    for i in range(per_row):
        dflat[pl.ds(i, height, stride=per_row), :] = dacc[last, :, i * LANE:(i + 1) * LANE]
    dflat[flat_rows:, :] = jnp.zeros((most, LANE), f32)
    wgrad_ref[...] = jnp.where(slot < count, dflat[pl.ds(offset, most), :], 0.0)

    for copy, cond in sends:
        if cond is None:
            copy.wait_send()
        else:
            pl.when(cond)(copy.wait_send)
    for z in range(outer):
        for k in range(1, inner):
            p_copy(z, k).wait_send()
    for i in range(last):
        for h in range(2):
            sum_copy(i, h).wait_send()


def fast_plan(mesh, hidden, key, wb):
    outer, inner, halves = (mesh.shape[n] for n in ("gx", "gy", "gz"))
    tokens, rows, width, most = hidden.shape[0], hidden.shape[1], key.shape[1], wb.shape[2]
    if inner != 4 or halves != 2 or outer < 3 or tokens != LANE or width % LANE or most % 8:
        return None
    per_row = width // LANE
    if rows % (outer * LANE):
        return None
    span = rows // outer
    lows, height = owner_windows(span * per_row, inner, most, per_row, span)
    if height < 32 or min(lows) < 0:
        return None
    held = 4 * owners_bytes(outer, inner, height, tokens) + 4 * outer * height * width * 4 + 8 * tokens * rows * 4
    if held > VMEM_BUDGET:
        return None
    return lows, height, per_row


def owners_bytes(outer, inner, height, tokens):
    return outer * inner * height * tokens * 2


def fast_shards(mesh, plan, hidden_in, norm_gain, normed_grad, key_grad, weight_blocks, block_count):
    lows, height, per_row = plan
    outer, inner = mesh.shape["gx"], mesh.shape["gy"]
    tokens, rows = hidden_in.shape
    width, most = key_grad.shape[1], weight_blocks.shape[2]
    model_width = rows * mesh.shape["gz"]
    flat_rows = height * per_row
    span = rows // outer
    pad = -(-max(min(j * most, span * per_row) - lows[j] * per_row for j in range(inner)) // 8) * 8
    dims = (outer, inner, model_width, most, per_row, height, pad)
    f32, bf16 = jnp.float32, jnp.bfloat16
    vmem, dma = pltpu.VMEM, pltpu.SemaphoreType.DMA
    in_vmem = pl.BlockSpec(memory_space=pltpu.VMEM)
    in_hbm = pl.BlockSpec(memory_space=pltpu.HBM)
    pieces = vmem((outer, inner, height, tokens), bf16)
    small = vmem((8, LANE), f32)
    smalls = vmem((inner, 8, LANE), f32)
    hgrad, wgrad = pl.pallas_call(
        functools.partial(fast_kernel, dims, lows),
        out_shape=(jax.ShapeDtypeStruct((tokens, rows), bf16), jax.ShapeDtypeStruct((most, LANE), f32)),
        in_specs=[pl.BlockSpec(memory_space=pltpu.SMEM), in_hbm, in_vmem] + [in_hbm] * 3,
        out_specs=(in_vmem, in_vmem),
        scratch_shapes=[
            vmem((tokens, rows), bf16), vmem((tokens, rows), bf16), vmem((most, LANE), bf16),
            vmem((inner, tokens, width), bf16), vmem((outer, height, width), bf16),
            pieces, pieces, pieces, pieces,
            vmem((span, tokens), f32), vmem((tokens, rows), f32), vmem((rows, LANE), f32),
            vmem((pad + max(flat_rows, most), LANE), f32), vmem((flat_rows, LANE), f32),
            vmem((outer, height, width), f32), vmem((outer, height, width), bf16),
            vmem((2 * outer, height, width), bf16), vmem((flat_rows + most, LANE), f32),
            small, small, smalls, smalls, smalls, small, small,
            dma((4,)), dma((inner,)), dma((inner,)),
            dma((outer, 2)), dma((outer, 2)), dma((outer, 2)),
            dma((outer, inner)), dma((outer, inner)), dma((outer, inner)), dma((outer, inner)),
            dma((outer, 2)), dma((2 * outer, 2)),
            dma((inner,)), dma((inner,)), dma((inner,)), dma((inner,)), dma((2,)), dma((2,)),
        ],
        compiler_params=pltpu.CompilerParams(
            collective_id=0, has_side_effects=True),
    )(block_count, hidden_in, norm_gain.reshape(1, rows), normed_grad, key_grad,
      weight_blocks.reshape(most, LANE))
    return hgrad, wgrad.reshape(1, 1, most, LANE)


def block_layout(counts, blocks, owners, most):
    ends = jnp.cumsum(counts)
    starts = ends - counts
    block_ids = jnp.arange(blocks, dtype=jnp.int32)
    owner = jnp.searchsorted(ends, block_ids, side="right")
    gather_index = owner * most + block_ids - starts[owner]
    slot_owner = jnp.arange(owners * most, dtype=jnp.int32) // most
    slot_within = jnp.arange(owners * most, dtype=jnp.int32) % most
    valid = slot_within < counts[slot_owner]
    source = jnp.clip(starts[slot_owner] + slot_within, 0, blocks - 1)
    return (gather_index, source, valid)


def select_rows(index, keep, rows):
    columns = jnp.arange(rows.shape[0], dtype=jnp.int32)
    onehot = (index[:, None] == columns[None, :]) & keep[:, None]
    if rows.dtype == jnp.bfloat16:
        picked = jnp.dot(onehot.astype(jnp.bfloat16), rows, preferred_element_type=jnp.float32)
        return picked.astype(jnp.bfloat16)
    return jnp.dot(
        onehot.astype(jnp.float32),
        rows,
        precision=lax.Precision.HIGHEST,
        preferred_element_type=jnp.float32,
    )


def select_groups(index, keep, rows):

    def one_group(items):
        return select_rows(items[0], items[1], items[2])

    return lax.map(one_group, (index, keep, rows))


def shards(hidden_in, norm_gain, normed_grad, key_grad, weight_blocks, block_count):
    outer_size = lax.axis_size("gx")
    inner_size = lax.axis_size("gy")
    owners = outer_size * inner_size
    most = weight_blocks.shape[2]
    group_slots_count = inner_size * most
    group_rows = hidden_in.shape[1]
    width = key_grad.shape[1]
    blocks = group_rows * width // 128
    group_blocks = (blocks + outer_size - 1) // outer_size
    model_width = group_rows * lax.axis_size("gz")
    gather_index, source, valid = block_layout(block_count[0], blocks, owners, most)
    outer_index = lax.axis_index("gx")
    padded_index = jnp.pad(gather_index, (0, outer_size * group_blocks - blocks), mode="edge")
    group_offsets = jnp.arange(outer_size, dtype=jnp.int32)[:, None]
    local_index = jnp.clip(
        padded_index.reshape(outer_size, group_blocks) - group_offsets * group_slots_count,
        0,
        group_slots_count - 1,
    )
    local_source = jnp.clip(
        source.reshape(outer_size, group_slots_count) - group_offsets * group_blocks,
        0,
        group_blocks - 1,
    )
    local_valid = valid.reshape(outer_size, group_slots_count)
    all_rows = jnp.ones((outer_size, group_blocks), dtype=bool)
    local_blocks = weight_blocks.reshape(most, 128)
    gathered = lax.all_gather(local_blocks, ("gx", "gy"), axis=0, tiled=True)
    dense = select_groups(
        local_index, all_rows, gathered.reshape(outer_size, group_slots_count, 128)
    )
    weight = dense.reshape(outer_size * group_blocks, 128)[:blocks].reshape(group_rows, width)
    hfloat = hidden_in.astype(jnp.float32)
    squares = lax.psum(jnp.sum(hfloat * hfloat, axis=1), "gz")
    rstd = lax.rsqrt(squares / model_width + EPS)
    normed = (hfloat * rstd[:, None] * norm_gain).astype(jnp.bfloat16)
    dnorm = normed_grad.astype(jnp.float32) + lax.dot_general(
        key_grad, weight, (((1,), (1,)), ((), ())), preferred_element_type=jnp.float32
    )
    proj = lax.psum(jnp.sum(norm_gain * dnorm * hfloat, axis=1), "gz")
    grad = norm_gain * dnorm * rstd[:, None] - hfloat * (rstd**3 * proj / model_width)[:, None]
    hidden_grad = grad.astype(jnp.bfloat16)
    dweight = lax.dot_general(
        normed, key_grad, (((0,), (0,)), ((), ())), preferred_element_type=jnp.float32
    )
    flat = dweight.reshape(blocks, 128)
    flat_padded = jnp.pad(flat, ((0, outer_size * group_blocks - blocks), (0, 0)))
    group_sum = lax.psum_scatter(flat_padded, "gx", scatter_dimension=0, tiled=True)
    slot_source = lax.dynamic_index_in_dim(local_source, outer_index, 0, keepdims=False)
    slot_valid = lax.dynamic_index_in_dim(local_valid, outer_index, 0, keepdims=False)
    slotted = select_rows(slot_source, slot_valid, group_sum)
    owned = lax.psum_scatter(slotted, "gy", scatter_dimension=0, tiled=True)
    return (hidden_grad, owned.reshape(1, 1, most, 128))


def solution(mesh):
    placed = (
        P(("gx", "gy"), "gz"),
        P("gz"),
        P(("gx", "gy"), "gz"),
        P(("gx", "gy"), None),
        P(("gx", "gy"), "gz", None, None),
        P("gz", None),
    )

    def body(*args):
        plan = fast_plan(mesh, args[0], args[3], args[4])
        if plan is None:
            return shards(*args)
        return fast_shards(mesh, plan, *args)

    return jax.shard_map(
        body,
        mesh=mesh,
        in_specs=placed,
        out_specs=(P(("gx", "gy"), "gz"), P(("gx", "gy"), "gz", None, None)),
        check_vma=False,
    )
```
